1024 devices in a mesh: replica: 64 (over z_hi, y, core), shard: 16 (over x, z_lo).
Axes of the slice: x: 4, y: 8, z: 16 (z_hi: 4, z_lo: 4; z = z_hi * 4 + z_lo), core: 2. Of those that a mesh axis runs over, the one named last changes fastest.
Arguments:
- inputs: bfloat16 [16384, 2048], P('replica'), may hold values from -16 to 16
- gate_pre: bfloat16 [16384, 8192], P('replica', 'shard'), may hold values from -8 to 8
- up_pre: bfloat16 [16384, 8192], P('replica', 'shard'), may hold values from -6 to 6
- hidden_grad: bfloat16 [16384, 8192], P('replica', 'shard'), may hold values from -16 to 16
- segment_ids: int32 [64, 256], P('replica'), may hold values from 0 to 15, never falling along the last dimension, each value on 1 to 64 neighbouring positions
- doc_weight: int32 [64, 16], P('replica'), may hold values from 1 to 13
- w_gate: bfloat16 [2048, 8192], P(None, 'shard'), may hold values from -0.0625 to 0.0625
- master: float32 [2048, 8192], P('replica', 'shard'), may hold values from -6 to 6
- moment: float32 [2048, 8192], P('replica', 'shard'), may hold values from -10 to 10
- second: float32 [2048, 8192], P('replica', 'shard'), may hold values from 0.5 to 20
Outputs:
- input_grad: bfloat16 [16384, 2048], P(('replica', 'shard'))
- up_grad: bfloat16 [16384, 8192], P('replica', 'shard')
- master_new: float32 [2048, 8192], P('replica', 'shard')
- moment_new: float32 [2048, 8192], P('replica', 'shard')
- second_new: float32 [2048, 8192], P('replica', 'shard')
The draws below stay inside these ranges and needn't reach their ends.
Inputs may be any that keep to these rules, and one draw needn't show every extreme that they name: `segment_ids`: within each group the documents occupy runs of positions numbered 0 to 15 in order, each at most 64 long.
All inputs are finite; a program needn't handle non-finite values.
Results may differ from the reference program's by a relative error of at most 0.0049.
Values sent between devices are 32-bit elements; how exact they have to be, the bound alone decides.
No kernel may reach another device: no remote copies, remote signals or barrier semaphores. Data moves between devices by JAX's collectives and lax.ppermute only.
A program may use at most 64 MiB of HBM per device.

```python
import math
import jax
import jax.numpy as jnp
import numpy as np
from jax import lax

DW = 2048
FF = 8192
SEGS = 16
GROUP_TOK = 256
TOKENS = 16384
N_REPLICA = 64


def draw_doc_weight(key, part):
    base_key = jax.random.fold_in(key, 11)
    start_key = jax.random.fold_in(key, 12)
    length_key = jax.random.fold_in(key, 13)
    base = jax.random.randint(base_key, (N_REPLICA, SEGS), 1, 4)
    groups = jnp.arange(N_REPLICA, dtype=jnp.int32)
    labels = jnp.arange(SEGS, dtype=jnp.int32)
    first_cell = (groups[:, None] == 0) & (labels[None, :] == 0)
    last_cell = (groups[:, None] == N_REPLICA - 1) & (labels[None, :] == 0)
    base = jnp.where(first_cell, 1, base)
    base = jnp.where(last_cell, 3, base)
    rising = 8 * groups // N_REPLICA
    window_start = jax.random.randint(start_key, (), 0, N_REPLICA)
    window_length = jax.random.randint(length_key, (), 0, N_REPLICA + 1)
    inside = (jnp.mod(groups - window_start, N_REPLICA) < window_length).astype(jnp.int32)
    inside = jnp.where(groups == 0, 0, inside)
    inside = jnp.where(groups == N_REPLICA - 1, 1, inside)
    return (base + rising[:, None] + 3 * inside[:, None]).astype(jnp.int32)


def spiked(result, stream_key, source, target, blocks, factor):
    def block_of(position):
        return (jnp.arange(result.shape[position]) // (result.shape[position] // blocks)).reshape((-1,) + (1,) * (result.ndim - 1 - position))

    one_side = jax.random.permutation(stream_key, blocks)[block_of(target)]
    other_side = (block_of(target) + blocks // 2) % blocks
    return jnp.where((block_of(source) == one_side) | (block_of(source) == other_side), factor * result, result)


def shard_levels(own_key, dims, cuts, smallest, largest):
    def one(axis_at, parts):
        steps = jax.random.uniform(jax.random.fold_in(jax.random.fold_in(own_key, 6), axis_at), (parts,), jnp.float32, smallest / len(cuts), largest / len(cuts))
        return jnp.repeat(jnp.exp(steps), dims[axis_at] // parts).reshape((-1,) + (1,) * (len(dims) - axis_at - 1))

    gain = one(*cuts[0])
    for cut in cuts[1:]:
        gain = gain * one(*cut)
    return gain


def split_up(count, total, limit, skew):
    loads = [(1 << 20) // math.isqrt(grade ** skew) + 1 for grade in range(2, count + 1)]
    surplus, holding = total - limit - (count - 1), [1] * (count - 1)
    while surplus > 0:
        free = [i for i in range(count - 1) if holding[i] < limit]
        mass, remaining = sum([loads[i] for i in free]), surplus
        for i in free:
            more = min(limit - holding[i], max(1, remaining * loads[i] // mass), surplus)
            holding[i] = holding[i] + more
            surplus = surplus - more
    return np.array([limit] + holding)


def ragged(stream_key, amount, total, bound, slope):
    if amount == 2:
        one = jax.random.randint(stream_key, (), max(1, total - bound), min(bound, total - 1) + 1)
        return jnp.stack([one, total - one])
    tallies = jnp.asarray(split_up(amount, total, bound, slope), jnp.int32)
    couples = (amount - 1) // 2
    giver, receiver = tallies[1:1 + 2 * couples:2], tallies[2:2 + 2 * couples:2]
    margin = jnp.minimum(giver - 1, bound - receiver)
    moved = jax.random.randint(jax.random.fold_in(stream_key, 1), (couples,), 0, 1 << 20) % (margin + 1)
    tallies = tallies.at[1:1 + 2 * couples:2].set(giver - moved).at[2:2 + 2 * couples:2].set(receiver + moved)
    return tallies[jax.random.permutation(jax.random.fold_in(stream_key, 2), amount)]


def noise(rng, shape, spread, reach, pieces=(), kind=jnp.bfloat16):
    loudness = shard_levels(rng, shape, pieces, -0.22, 0.18) if pieces else 1.0
    values = jax.random.normal(rng, shape, jnp.float32) * spread * loudness
    return jnp.minimum(jnp.maximum(values, -reach), reach).astype(kind)


def heavy_noise(rng, shape, deviation, limit, split, heavy, kind=jnp.bfloat16):
    drawn = deviation * jax.random.normal(rng, shape, jnp.float32)
    if split:
        drawn = drawn * shard_levels(rng, shape, split, -0.22, 0.18)
    return jnp.clip(spiked(drawn, jax.random.fold_in(rng, 3), *heavy), -limit, limit).astype(kind)


def setup_inputs(seed: int = 0) -> dict:
    keys = jax.random.split(jax.random.key(seed), 11)
    return {
        "inputs": heavy_noise(keys[0], (TOKENS, DW), 1.0, 16.0, ((0, 64),), (0, 1, 64, 4.0)),
        "gate_pre": noise(keys[1], (TOKENS, FF), 2.0, 8.0, ((0, 64), (1, 16))),
        "up_pre": noise(keys[2], (TOKENS, FF), 1.0, 6.0, ((0, 64), (1, 16))),
        "hidden_grad": heavy_noise(keys[3], (TOKENS, FF), 1.0, 16.0, ((0, 64), (1, 16)), (1, 0, 64, 4.0)),
        "segment_ids": jax.vmap(lambda own: jnp.searchsorted(jnp.cumsum(ragged(own, SEGS, GROUP_TOK, GROUP_TOK // 4, 2)), jnp.arange(GROUP_TOK), side="right"))(jax.random.split(keys[4], N_REPLICA)).reshape((N_REPLICA, GROUP_TOK)).astype(jnp.int32),
        "doc_weight": draw_doc_weight(jax.random.fold_in(keys[10], 71), 0),
        "w_gate": noise(keys[6], (DW, FF), FF ** -0.5, 0.0625, ((1, 16),)),
        "master": noise(keys[7], (DW, FF), 1.0, 6.0, ((0, 64), (1, 16)), jnp.float32),
        "moment": noise(keys[8], (DW, FF), 2.0, 10.0, ((0, 64), (1, 16)), jnp.float32),
        "second": jnp.clip(jnp.exp(math.log(20.0) - 3.6888795 * jax.random.uniform(keys[9], (DW, FF), jnp.float32) ** shard_levels(keys[9], (DW, FF), ((0, 64), (1, 16)), -0.2, 0.2)), 0.5, 20.0),
    }


def token_weights(segment_ids, doc_weight):
    labels = jnp.arange(doc_weight.shape[1], dtype=jnp.int32)
    onehot = segment_ids[:, :, None] == labels[None, None, :]
    return lax.optimization_barrier(jnp.sum(jnp.where(onehot, doc_weight[:, None, :], 0), axis=2)).astype(jnp.int32)

def reference(inputs, gate_pre, up_pre, hidden_grad, segment_ids, doc_weight, w_gate, master, moment, second):
    weights = token_weights(segment_ids, doc_weight)
    total = jnp.sum(weights).astype(jnp.int32)
    total_f = total.astype(jnp.float32)
    scale = jnp.float32(TOKENS) / total_f
    group_scale = jnp.float32(GROUP_TOK) / total_f
    stacked = (inputs.reshape(N_REPLICA, GROUP_TOK, DW), gate_pre.reshape(N_REPLICA, GROUP_TOK, FF), up_pre.reshape(N_REPLICA, GROUP_TOK, FF), hidden_grad.reshape(N_REPLICA, GROUP_TOK, FF), weights)

    def one_group(accum, block):
        rows, gate_blk, up_blk, grad_blk, weight_blk = block
        gate_f = gate_blk.astype(jnp.float32)
        sigmoid_gate = jax.nn.sigmoid(gate_f)
        weighted = grad_blk.astype(jnp.float32) * weight_blk.astype(jnp.float32)[:, None]
        gate_raw = (weighted * up_blk.astype(jnp.float32) * sigmoid_gate * (1.0 + gate_f * (1.0 - sigmoid_gate))).astype(jnp.bfloat16)
        up_out = (weighted * gate_f * sigmoid_gate * scale).astype(jnp.bfloat16)
        input_part = lax.dot_general(gate_raw, w_gate, (((1,), (1,)), ((), ())), preferred_element_type=jnp.float32)
        input_out = (input_part * scale).astype(jnp.bfloat16)
        accum = accum + lax.dot_general(rows, gate_raw, (((0,), (0,)), ((), ())), preferred_element_type=jnp.float32)
        return (accum, (input_out, up_out))
    start = jnp.zeros((DW, FF), jnp.float32)
    weight_raw, (input_grad, up_grad) = lax.scan(one_group, start, stacked)
    grad = weight_raw * group_scale
    moment_new = 0.9 * moment + 0.1 * grad
    second_new = 0.95 * second + 0.05 * grad * grad
    first_fix = moment_new / (1.0 - 0.9 ** 8)
    second_fix = second_new / (1.0 - 0.95 ** 8)
    master_new = master - 0.003 * (first_fix / (jnp.sqrt(second_fix) + 1e-08) + 0.1 * master)
    return (input_grad.reshape(TOKENS, DW), up_grad.reshape(TOKENS, FF), master_new, moment_new, second_new)
```

```python
import functools
import math

import jax
import jax.numpy as jnp
from jax import lax
from jax.experimental import pallas as pl
from jax.experimental.pallas import tpu as pltpu
from jax.sharding import Mesh
from jax.sharding import PartitionSpec as P

REPLICA = ("z_hi", "y", "core")
SHARD = ("x", "z_lo")


def shift(size, by):
    return [(i, (i + by) % size) for i in range(size)]


def silu_parts(gate_pre, hidden_grad, weights):
    gate = gate_pre.astype(jnp.float32)
    sig = 1.0 / (1.0 + jnp.exp(-gate))
    return gate, sig, hidden_grad.astype(jnp.float32) * weights


def weight_grad_kernel(
    where_ref, inputs_hbm, gate_hbm, up_hbm, hidden_hbm, seg_hbm, doc_hbm,
    send_far, send_rest, keep_far, keep_rest, raw_hbm, weights_hbm,
    full_ref, inputs_ref, gate_ref, up_ref, hidden_ref, seg_ref, doc_ref, raw_ref, weights_ref, tail_ref,
    arrived, left,
):
    pairs = (
        (seg_hbm, seg_ref), (doc_hbm, doc_ref), (gate_hbm, gate_ref), (hidden_hbm, hidden_ref),
        (up_hbm, up_ref), (inputs_hbm, inputs_ref),
    )
    copies = [pltpu.make_async_copy(a, b, arrived.at[i]) for i, (a, b) in enumerate(pairs)]
    for copy in copies:
        copy.start()
    for copy in copies[:2]:
        copy.wait()
    y, core = where_ref[0], where_ref[1]
    layers, blocks, cores, rows, ff = full_ref.shape
    out = []

    def put(src, dst):
        copy = pltpu.make_async_copy(src, dst, left.at[len(out)])
        copy.start()
        out.append(copy)

    segs = doc_ref.shape[1]
    tokens = seg_ref.shape[1]
    doc = doc_ref[...].astype(jnp.float32)
    row = lax.broadcasted_iota(jnp.int32, (segs, segs), 0)
    col = lax.broadcasted_iota(jnp.int32, (segs, segs), 1)
    doc_col = jnp.sum(jnp.where(row == col, doc, 0.0), axis=1, keepdims=True)
    label = lax.broadcasted_iota(jnp.int32, (segs, tokens), 0)
    onehot = jnp.where(label == seg_ref[...], 1.0, 0.0)
    tail_ref[...] = jnp.full(tail_ref.shape, jnp.sum(onehot * doc_col), jnp.float32)
    wide = lax.dot_general(
        onehot.astype(jnp.bfloat16),
        jnp.broadcast_to(doc_col, (segs, 128)).astype(jnp.bfloat16),
        (((0,), (0,)), ((), ())),
        preferred_element_type=jnp.float32,
    )
    weights_ref[...] = wide
    weights = wide[:, :1]
    for copy in copies[2:5]:
        copy.wait()
    gate, sig, weighted = silu_parts(gate_ref[...], hidden_ref[...], weights)
    up = up_ref[...].astype(jnp.float32)
    raw = (weighted * up * sig * (1.0 + gate * (1.0 - sig))).astype(jnp.bfloat16)
    raw_ref[...] = raw
    per = blocks * cores * rows
    copies[5].wait()
    parts = [
        (send_far, send_rest, 1 - core),
        (keep_far, keep_rest, core),
    ]
    for z in range(layers):
        part = lax.dot_general(
            inputs_ref[:, z * per : (z + 1) * per], raw, (((0,), (0,)), ((), ())),
            preferred_element_type=jnp.float32,
        )
        full_ref[z] = part.reshape(blocks, cores, rows, ff)
        lines = pl.ds(z * rows, rows)
        for far, rest, side in parts:
            for k in (blocks // 2, *range(blocks // 2), *range(blocks // 2 + 1, blocks)):
                src = full_ref.at[z, lax.rem(y + k, blocks), side]
                put(src, far.at[lines] if k == blocks // 2 else rest.at[spot(k, blocks), lines])
        if z == 0:
            lines = pl.ds(layers * rows, 8)
            for far, rest, _ in parts:
                put(tail_ref, far.at[lines])
                for k in range(blocks - 1):
                    put(tail_ref, rest.at[k, lines])
            put(raw_ref, raw_hbm)
            put(weights_ref, weights_hbm)
    for copy in out:
        copy.wait()


def spot(k, blocks):
    return k if k < blocks // 2 else k - 1


def input_part_kernel(
    raw_hbm, w_hbm, gate_hbm, hidden_hbm, weights_hbm, out_hbm, up_hbm,
    raw_ref, w_ref, gate_ref, hidden_ref, weights_ref, out_ref, up_ref, arrived, left,
):
    pairs = (
        (raw_hbm, raw_ref), (w_hbm, w_ref), (weights_hbm, weights_ref), (gate_hbm, gate_ref),
        (hidden_hbm, hidden_ref),
    )
    copies = [pltpu.make_async_copy(a, b, arrived.at[i]) for i, (a, b) in enumerate(pairs)]
    for copy in copies:
        copy.start()
    for copy in copies[:2]:
        copy.wait()
    cuts = left.shape[0] - 1
    step = raw_ref.shape[0] // cuts
    out = []
    for i in range(cuts):
        lines = pl.ds(i * step, step)
        out_ref[lines] = lax.dot_general(
            raw_ref[lines], w_ref[...], (((1,), (1,)), ((), ())), preferred_element_type=jnp.float32
        )
        out.append(pltpu.make_async_copy(out_ref.at[lines], out_hbm.at[lines], left.at[i]))
        out[-1].start()
    for copy in copies[2:]:
        copy.wait()
    gate, sig, weighted = silu_parts(gate_ref[...], hidden_ref[...], weights_ref[:, :1])
    up_ref[...] = weighted * gate * sig
    out.append(pltpu.make_async_copy(up_ref, up_hbm, left.at[cuts]))
    out[-1].start()
    for copy in out:
        copy.wait()


def far_kernel(cut, own_ref, other_ref, ahead_ref, behind_ref):
    ahead_ref[...] = own_ref[:cut] + other_ref[:cut]
    behind_ref[...] = own_ref[cut:] + other_ref[cut:]


def rest_kernel(own_ref, other_ref, out_ref):
    out_ref[...] = own_ref[...] + other_ref[...]


def hop_kernel(up_block, down_block, terms_ref, came_up_ref, came_down_ref, ahead_ref, behind_ref):
    length = terms_ref.shape[1]
    for out, came, block, low in (
        (ahead_ref, came_up_ref, up_block, 0),
        (behind_ref, came_down_ref, down_block, length - came_down_ref.shape[0]),
    ):
        high = low + came.shape[0]
        out[low:high] = terms_ref[block, low:high] + came[...]
        for lo, hi in ((0, low), (high, length)):
            if hi > lo:
                out[lo:hi] = terms_ref[block, lo:hi]


def last_kernel(terms_ref, came_up_ref, came_down_ref, out_ref):
    layers, rows = out_ref.shape[0], out_ref.shape[1] - 8
    for z in range(layers + 1):
        part = pl.ds(z * rows, rows if z < layers else 8)
        block = terms_ref[0, part] + (came_up_ref[part] + came_down_ref[part])
        if z < layers:
            out_ref[z, :rows] = block
        else:
            for k in range(layers):
                out_ref[k, rows:] = block


def fold_kernel(pieces_ref, out_ref):
    total = pieces_ref[0]
    for k in range(1, pieces_ref.shape[0]):
        total = total + pieces_ref[k]
    out_ref[...] = total


def last_step_kernel(
    replicas, group_rows, pieces_ref, input_ref, up_ref, master_ref, moment_ref, second_ref,
    input_grad_ref, up_grad_ref, master_out, moment_out, second_out,
):
    rows = master_ref.shape[0]
    summed, input_sum = pieces_ref[0], input_ref[0]
    for k in range(1, pieces_ref.shape[0]):
        summed = summed + pieces_ref[k]
    for k in range(1, input_ref.shape[0]):
        input_sum = input_sum + input_ref[k]
    total = summed[rows : rows + 1, :1]
    scale = jnp.float32(group_rows * replicas) / total
    group_scale = jnp.float32(group_rows) / total
    input_grad_ref[...] = (input_sum * scale).astype(jnp.bfloat16)
    up_grad_ref[...] = (up_ref[...] * scale).astype(jnp.bfloat16)
    grad = summed[:rows] * group_scale
    moment = 0.9 * moment_ref[...] + 0.1 * grad
    second = 0.95 * second_ref[...] + 0.05 * grad * grad
    moment_out[...] = moment
    second_out[...] = second
    first_fix = moment / (1.0 - 0.9**8)
    second_fix = second / (1.0 - 0.95**8)
    master = master_ref[...]
    master_out[...] = master - 0.003 * (first_fix / (jnp.sqrt(second_fix) + 1e-08) + 0.1 * master)


def local(kernel, outs, *args, flops=0):
    vmem = pl.BlockSpec(memory_space=pltpu.VMEM)
    moved = sum(math.prod(a.shape) * a.dtype.itemsize for a in (*args, *outs))
    single = len(outs) == 1
    return pl.pallas_call(
        kernel,
        out_shape=outs[0] if single else tuple(outs),
        in_specs=[vmem] * len(args),
        out_specs=vmem if single else (vmem,) * len(outs),
        compiler_params=pltpu.CompilerParams(vmem_limit_bytes=16 * 2**20),
        cost_estimate=pl.CostEstimate(flops=max(flops, moved), bytes_accessed=moved, transcendentals=0),
    )(*args)


def weight_grad(where, inputs, gate_pre, up_pre, hidden_grad, segment_ids, doc_weight, sizes):
    layers, blocks, cores = sizes
    tokens, dw = inputs.shape
    ff = gate_pre.shape[1]
    rows = dw // (layers * blocks * cores)
    far, rest = f32(layers * rows + 8, ff), f32(blocks - 1, layers * rows + 8, ff)
    hbm = pl.BlockSpec(memory_space=pl.ANY)
    args = (inputs, gate_pre, up_pre, hidden_grad, segment_ids, doc_weight)
    return pl.pallas_call(
        weight_grad_kernel,
        out_shape=(far, rest, far, rest, bf16(tokens, ff), f32(tokens, 128)),
        in_specs=[pl.BlockSpec(memory_space=pltpu.SMEM)] + [hbm] * 6,
        out_specs=(hbm,) * 6,
        scratch_shapes=[pltpu.VMEM((layers, blocks, cores, rows, ff), jnp.float32)]
        + [pltpu.VMEM(a.shape, a.dtype) for a in args]
        + [
            pltpu.VMEM((tokens, ff), jnp.bfloat16),
            pltpu.VMEM((tokens, 128), jnp.float32),
            pltpu.VMEM((8, ff), jnp.float32),
            pltpu.SemaphoreType.DMA((6,)),
            pltpu.SemaphoreType.DMA((2 * (layers + 1) * blocks + 2,)),
        ],
        compiler_params=pltpu.CompilerParams(vmem_limit_bytes=56 * 2**20),
        cost_estimate=pl.CostEstimate(
            flops=2 * tokens * dw * ff, bytes_accessed=14 * 2**20, transcendentals=tokens * ff
        ),
        name="weight_grad",
    )(where, *args)


def input_part(raw, w_gate, gate_pre, hidden_grad, wide):
    tokens, ff = raw.shape
    dw, cuts = w_gate.shape[0], 4
    hbm = pl.BlockSpec(memory_space=pl.ANY)
    args = (raw, w_gate, gate_pre, hidden_grad, wide)
    outs = (f32(tokens, dw), f32(tokens, ff))
    return pl.pallas_call(
        input_part_kernel,
        out_shape=outs,
        in_specs=[hbm] * 5,
        out_specs=(hbm,) * 2,
        scratch_shapes=[pltpu.VMEM(a.shape, a.dtype) for a in (*args, *outs)]
        + [pltpu.SemaphoreType.DMA((5,)), pltpu.SemaphoreType.DMA((cuts + 1,))],
        compiler_params=pltpu.CompilerParams(vmem_limit_bytes=56 * 2**20),
        cost_estimate=pl.CostEstimate(
            flops=2 * tokens * dw * ff, bytes_accessed=7 * 2**20, transcendentals=tokens * ff
        ),
        name="input_part",
    )(*args)


def f32(*shape):
    return jax.ShapeDtypeStruct(shape, jnp.float32)


def bf16(*shape):
    return jax.ShapeDtypeStruct(shape, jnp.bfloat16)


def ring_reduce(far, terms, layers):
    length, ff = far[0].shape
    size = lax.axis_size("y")
    half, cut = size // 2, (length // 2) // 8 * 8
    up, down = shift(size, 1), shift(size, -1)
    ahead, behind = local(functools.partial(far_kernel, cut), [f32(cut, ff), f32(length - cut, ff)], *far)
    for step in range(half - 1, -1, -1):
        ahead = lax.ppermute(ahead, "y", up)
        behind = lax.ppermute(behind, "y", down)
        if step == half - 1:
            terms = terms()
        if step:
            ahead, behind = local(
                functools.partial(hop_kernel, spot(step, size), spot(size - step, size)),
                [f32(length, ff), f32(length, ff)], terms, ahead, behind,
            )
    return local(last_kernel, [f32(layers, (length - 8) // layers + 8, ff)], terms, ahead, behind)


def on_device(
    inputs, gate_pre, up_pre, hidden_grad, segment_ids, doc_weight, w_gate, master, moment, second
):
    group_rows, dw = inputs.shape
    ff = gate_pre.shape[1]
    replicas = lax.axis_size(REPLICA)
    layers, blocks, cores = (lax.axis_size(a) for a in REPLICA)
    nx, nz = (lax.axis_size(a) for a in SHARD)
    own_rows = group_rows // (nx * nz)
    where = jnp.stack([lax.axis_index("y"), lax.axis_index("core")]).astype(jnp.int32)
    send_far, send_rest, keep_far, keep_rest, raw, wide = weight_grad(
        where, inputs, gate_pre, up_pre, hidden_grad, segment_ids, doc_weight, (layers, blocks, cores)
    )
    got_far = lax.ppermute(send_far, "core", shift(cores, 1))
    got_rest = lax.ppermute(send_rest, "core", shift(cores, 1))
    part, up_part = input_part(raw, w_gate, gate_pre, hidden_grad, wide)
    over_x = lax.all_to_all(part.reshape(nx, nz * own_rows, dw), "x", 0, 0, tiled=True)
    folded = local(fold_kernel, [f32(nz * own_rows, dw)], over_x)
    over_z = lax.all_to_all(folded.reshape(nz, own_rows, dw), "z_lo", 0, 0, tiled=True)
    mine = ring_reduce((keep_far, got_far), lambda: local(rest_kernel, [f32(*keep_rest.shape)], keep_rest, got_rest), layers)
    pieces = lax.all_to_all(mine, "z_hi", 0, 0, tiled=True)
    state = f32(*master.shape)
    return local(
        functools.partial(last_step_kernel, replicas, group_rows),
        [bf16(own_rows, dw), bf16(group_rows, ff), state, state, state],
        pieces, over_z, up_part, master, moment, second,
    )


def solution(mesh):
    split = Mesh(mesh.devices.reshape(4, 8, 2, 4, 4), REPLICA + SHARD)
    return jax.shard_map(
        on_device,
        mesh=split,
        in_specs=(
            P(REPLICA, None),
            P(REPLICA, SHARD),
            P(REPLICA, SHARD),
            P(REPLICA, SHARD),
            P(REPLICA, None),
            P(REPLICA, None),
            P(None, SHARD),
            P(REPLICA, SHARD),
            P(REPLICA, SHARD),
            P(REPLICA, SHARD),
        ),
        out_specs=(
            P(REPLICA + SHARD, None),
            P(REPLICA, SHARD),
            P(REPLICA, SHARD),
            P(REPLICA, SHARD),
            P(REPLICA, SHARD),
        ),
        check_vma=False,
    )
```

```python
import functools
import math

import jax
import jax.numpy as jnp
from jax import lax
from jax.experimental import pallas as pl
from jax.experimental.pallas import tpu as pltpu
from jax.sharding import Mesh
from jax.sharding import PartitionSpec as P

REPLICA = ("z_hi", "y", "core")
SHARD = ("x", "z_lo")


def swap(cores):
    return [(i, (i + 1) % cores) for i in range(cores)]


def one_way(size, cores, turn=1):
    ways = [turn if c % 2 == 0 else -turn for c in range(cores)]
    return [(i * cores + c, (i + ways[c]) % size * cores + c) for i in range(size) for c in range(cores)]


def silu_parts(gate_pre, hidden_grad, weights):
    gate = gate_pre.astype(jnp.float32)
    sig = 1.0 / (1.0 + jnp.exp(-gate))
    return gate, sig, hidden_grad.astype(jnp.float32) * weights


def front_kernel(
    inputs_hbm, gate_hbm, up_hbm, hidden_hbm, seg_hbm, doc_hbm, w_hbm,
    send_far, send_rest, keep_far, keep_rest, part_hbm, up_part_hbm,
    inputs_ref, gate_ref, up_ref, hidden_ref, seg_ref, doc_ref, w_ref,
    full_ref, tail_ref, part_ref, up_part_ref, arrived, left,
):
    pairs = (
        (seg_hbm, seg_ref), (doc_hbm, doc_ref), (gate_hbm, gate_ref), (hidden_hbm, hidden_ref),
        (up_hbm, up_ref), (inputs_hbm, inputs_ref), (w_hbm, w_ref),
    )
    copies = [pltpu.make_async_copy(a, b, arrived.at[i]) for i, (a, b) in enumerate(pairs)]
    for copy in copies:
        copy.start()
    y, core = lax.axis_index("y"), lax.axis_index("core")
    layers, blocks, cores, rows, ff = full_ref.shape
    half = blocks // 2
    out = []

    def put(src, dst):
        copy = pltpu.make_async_copy(src, dst, left.at[len(out)])
        copy.start()
        out.append(copy)

    for copy in copies[:2]:
        copy.wait()
    segs = doc_ref.shape[1]
    tokens = seg_ref.shape[1]
    doc = doc_ref[...].astype(jnp.float32)
    row = lax.broadcasted_iota(jnp.int32, (segs, segs), 0)
    col = lax.broadcasted_iota(jnp.int32, (segs, segs), 1)
    doc_col = jnp.sum(jnp.where(row == col, doc, 0.0), axis=1, keepdims=True)
    label = lax.broadcasted_iota(jnp.int32, (segs, tokens), 0)
    onehot = jnp.where(label == seg_ref[...], 1.0, 0.0)
    tail_ref[...] = jnp.full(tail_ref.shape, jnp.sum(onehot * doc_col), jnp.float32)
    wide = lax.dot_general(
        onehot.astype(jnp.bfloat16),
        jnp.broadcast_to(doc_col, (segs, 128)).astype(jnp.bfloat16),
        (((0,), (0,)), ((), ())),
        preferred_element_type=jnp.float32,
    )
    weights = wide[:, :1]
    for copy in copies[2:5]:
        copy.wait()
    gate, sig, weighted = silu_parts(gate_ref[...], hidden_ref[...], weights)
    up = up_ref[...].astype(jnp.float32)
    raw = (weighted * up * sig * (1.0 + gate * (1.0 - sig))).astype(jnp.bfloat16)
    up_part_ref[...] = weighted * gate * sig
    put(up_part_ref, up_part_hbm)
    per = blocks * cores * rows
    sides = []
    for far, rest, side in ((send_far, send_rest, 1 - core), (keep_far, keep_rest, core)):
        way = 1 - 2 * side
        todo = [(far, None, y + half, side)]
        for k in range(half - 1, 0, -1):
            place = 2 * (half - 1 - k)
            todo.append((rest, place, y + way * k, side))
            todo.append((rest, place + 1, y + way * k, 1 - side))
        todo.append((rest, blocks - 2, y, side))
        sides += todo
    copies[5].wait()
    for z in range(layers):
        part = lax.dot_general(
            inputs_ref[:, z * per : (z + 1) * per], raw, (((0,), (0,)), ((), ())),
            preferred_element_type=jnp.float32,
        )
        full_ref[z] = part.reshape(blocks, cores, rows, ff)
        lines = pl.ds(z * rows, rows)
        for ref, place, target, side in sides:
            target = lax.rem(target + blocks, blocks)
            if place is None:
                ref[lines] = full_ref[z, target, side]
            else:
                put(full_ref.at[z, target, side], ref.at[place, lines])
        if z == 0:
            lines = pl.ds(layers * rows, 8)
            for ref, place, _, _ in sides:
                if place is None:
                    ref[lines] = tail_ref[...]
                else:
                    put(tail_ref, ref.at[place, lines])
    copies[6].wait()
    step = w_ref.shape[0] // 4
    for i in range(4):
        cols = pl.ds(i * step, step)
        part_ref[:, cols] = lax.dot_general(
            raw, w_ref[cols], (((1,), (1,)), ((), ())), preferred_element_type=jnp.float32
        )
        put(part_ref.at[:, cols], part_hbm.at[:, cols])
    for copy in out:
        copy.wait()


def add_kernel(own_ref, other_ref, out_ref):
    out_ref[...] = own_ref[...] + other_ref[...]


def rest_kernel(own_ref, other_ref, terms_ref, *first_refs):
    for place, block in enumerate((0, 3, 2, 6)):
        terms_ref[place] = own_ref[block] + other_ref[block]
    for ref, block in zip(first_refs, (1, 5, 4)):
        ref[...] = own_ref[block] + other_ref[block]


def hop_kernel(block, terms_ref, came_ref, out_ref):
    out_ref[...] = terms_ref[block] + came_ref[...]


def cut_kernel(terms_ref, came_ref, next_ref, swapped_ref, far_ref, back_ref, near_ref, mine_ref):
    layers = lax.axis_size("z_hi")
    block = terms_ref.shape[0] - 1
    rows = (terms_ref.shape[1] - 8) // layers
    z, core = lax.axis_index("z_hi"), lax.axis_index("core")
    way = 1 - 2 * core
    wide = terms_ref.shape[2] // 128
    tail = pl.ds(layers * rows, 8)

    def total(part, cols):
        own = came_ref[part, cols] + next_ref[part, cols]
        return terms_ref[block, part, cols] + own + swapped_ref[part, cols]

    count = total(tail, pl.ds(0, 128))
    for out, target in ((far_ref, z + layers // 2), (back_ref, z - way), (near_ref, z + way), (mine_ref, z)):
        start = pl.multiple_of(lax.rem(target + layers, layers) * rows, rows)
        part = pl.ds(start, rows)
        for c in range(wide):
            out[c * rows : (c + 1) * rows] = total(part, pl.ds(c * 128, 128))
        out[wide * rows :] = count


def fold_kernel(pieces_hbm, out_hbm, pieces_ref, out_ref, arrived, left):
    n, rows = pieces_ref.shape[0], pieces_ref.shape[1]
    cuts = left.shape[0]
    step = rows // cuts
    copies, out = [], []
    for i in range(cuts):
        lines = pl.ds(i * step, step)
        copies.append(
            pltpu.make_async_copy(pieces_hbm.at[:, lines], pieces_ref.at[:, lines], arrived.at[i])
        )
        copies[-1].start()
    for i in range(cuts):
        lines = pl.ds(i * step, step)
        copies[i].wait()
        total = pieces_ref[0, lines]
        for k in range(1, n):
            total = total + pieces_ref[k, lines]
        out_ref[lines] = total
        out.append(pltpu.make_async_copy(out_ref.at[lines], out_hbm.at[lines], left.at[i]))
        out[-1].start()
    for copy in out:
        copy.wait()


def state_kernel(master_ref, moment_ref, second_ref, master_out, moment_out, second_out):
    master_out[...] = master_ref[...]
    moment_out[...] = 0.9 * moment_ref[...]
    second_out[...] = 0.95 * second_ref[...]


def last_step_kernel(
    replicas, group_rows, mine_ref, came_ref, back_ref, input_ref, up_ref, master_ref, moment_ref, second_ref,
    input_grad_ref, up_grad_ref, master_out, moment_out, second_out,
):
    rows, ff = master_ref.shape
    wide = ff // 128
    tail = pl.ds(wide * rows, 8)
    count = mine_ref[tail] + came_ref[tail] + back_ref[tail]
    total = count[:1, :1]
    scale = jnp.float32(group_rows * replicas) / total
    group_scale = jnp.float32(group_rows) / total
    input_sum = input_ref[0]
    for k in range(1, input_ref.shape[0]):
        input_sum = input_sum + input_ref[k]
    input_grad_ref[...] = (input_sum * scale).astype(jnp.bfloat16)
    up_grad_ref[...] = (up_ref[...] * scale).astype(jnp.bfloat16)
    for c in range(wide):
        part, cols = pl.ds(c * rows, rows), pl.ds(c * 128, 128)
        grad = (mine_ref[part] + came_ref[part] + back_ref[part]) * group_scale
        moment = moment_ref[:, cols] + 0.1 * grad
        second = second_ref[:, cols] + 0.05 * grad * grad
        moment_out[:, cols] = moment
        second_out[:, cols] = second
        first_fix = moment / (1.0 - 0.9**8)
        second_fix = second / (1.0 - 0.95**8)
        master = master_ref[:, cols]
        master_out[:, cols] = master - 0.003 * (
            first_fix / (jnp.sqrt(second_fix) + 1e-08) + 0.1 * master
        )


def local(kernel, outs, *args, flops=0):
    vmem = pl.BlockSpec(memory_space=pltpu.VMEM)
    moved = sum(math.prod(a.shape) * a.dtype.itemsize for a in (*args, *outs))
    single = len(outs) == 1
    return pl.pallas_call(
        kernel,
        out_shape=outs[0] if single else tuple(outs),
        in_specs=[vmem] * len(args),
        out_specs=vmem if single else (vmem,) * len(outs),
        compiler_params=pltpu.CompilerParams(vmem_limit_bytes=16 * 2**20),
        cost_estimate=pl.CostEstimate(flops=max(flops, moved), bytes_accessed=moved, transcendentals=0),
    )(*args)


def front(inputs, gate_pre, up_pre, hidden_grad, segment_ids, doc_weight, w_gate, sizes):
    layers, blocks, cores = sizes
    tokens, dw = inputs.shape
    ff = gate_pre.shape[1]
    rows = dw // (layers * blocks * cores)
    far, rest = f32(layers * rows + 8, ff), f32(blocks - 1, layers * rows + 8, ff)
    hbm, vmem = pl.BlockSpec(memory_space=pl.ANY), pl.BlockSpec(memory_space=pltpu.VMEM)
    args = (inputs, gate_pre, up_pre, hidden_grad, segment_ids, doc_weight, w_gate)
    return pl.pallas_call(
        front_kernel,
        out_shape=(far, rest, far, rest, f32(tokens, dw), f32(tokens, ff)),
        in_specs=[hbm] * 7,
        out_specs=(vmem, hbm, vmem, hbm, hbm, hbm),
        scratch_shapes=[pltpu.VMEM(a.shape, a.dtype) for a in args]
        + [
            pltpu.VMEM((layers, blocks, cores, rows, ff), jnp.float32),
            pltpu.VMEM((8, ff), jnp.float32),
            pltpu.VMEM((tokens, dw), jnp.float32),
            pltpu.VMEM((tokens, ff), jnp.float32),
            pltpu.SemaphoreType.DMA((7,)),
            pltpu.SemaphoreType.DMA((2 * (layers + 1) * blocks + 5,)),
        ],
        compiler_params=pltpu.CompilerParams(vmem_limit_bytes=56 * 2**20),
        cost_estimate=pl.CostEstimate(
            flops=4 * tokens * dw * ff, bytes_accessed=14 * 2**20, transcendentals=tokens * ff
        ),
        name="front",
    )(*args)


def fold(pieces):
    hbm = pl.BlockSpec(memory_space=pl.ANY)
    out = f32(*pieces.shape[1:])
    cuts = 4
    return pl.pallas_call(
        fold_kernel,
        out_shape=out,
        in_specs=[hbm],
        out_specs=hbm,
        scratch_shapes=[pltpu.VMEM(a.shape, a.dtype) for a in (pieces, out)]
        + [pltpu.SemaphoreType.DMA((cuts,)), pltpu.SemaphoreType.DMA((cuts,))],
        compiler_params=pltpu.CompilerParams(vmem_limit_bytes=56 * 2**20),
        cost_estimate=pl.CostEstimate(flops=2**22, bytes_accessed=5 * 2**19, transcendentals=0),
        name="fold_x",
    )(pieces)


def f32(*shape):
    return jax.ShapeDtypeStruct(shape, jnp.float32)


def bf16(*shape):
    return jax.ShapeDtypeStruct(shape, jnp.bfloat16)


def on_device(
    inputs, gate_pre, up_pre, hidden_grad, segment_ids, doc_weight, w_gate, master, moment, second
):
    group_rows, dw = inputs.shape
    rows, ff = master.shape
    replicas = lax.axis_size(REPLICA)
    layers, blocks, cores = (lax.axis_size(a) for a in REPLICA)
    nx, nz = (lax.axis_size(a) for a in SHARD)
    own_rows = group_rows // (nx * nz)
    send_far, send_rest, keep_far, keep_rest, part, up_part = front(
        inputs, gate_pre, up_pre, hidden_grad, segment_ids, doc_weight, w_gate, (layers, blocks, cores)
    )
    over_x = lax.all_to_all(part.reshape(nx, nz * own_rows, dw), "x", 0, 0, tiled=True)
    got_far = lax.ppermute(send_far, "core", swap(cores))
    got_rest = lax.ppermute(send_rest, "core", swap(cores))

    block = f32(layers * rows + 8, ff)
    ring, one, two = ("y", "core"), one_way(blocks, cores), one_way(blocks, cores, 2)
    own = local(add_kernel, [block], keep_far, got_far)
    own = lax.ppermute(own, ring, one)
    terms, other, other_next, own_next = local(
        rest_kernel, [f32(4, layers * rows + 8, ff)] + [block] * 3, keep_rest, got_rest
    )
    other = lax.ppermute(other, ring, one)
    other_next = lax.ppermute(other_next, ring, one)
    own = local(functools.partial(hop_kernel, 0), [block], terms, own)
    own = lax.ppermute(own, ring, one)
    own_next = lax.ppermute(own_next, ring, one)
    other = local(functools.partial(hop_kernel, 1), [block], terms, other)
    other = lax.ppermute(other, ring, two)
    own = local(functools.partial(hop_kernel, 2), [block], terms, own)
    own = lax.ppermute(own, ring, two)
    other = local(add_kernel, [block], other, other_next)
    other = lax.ppermute(other, "core", swap(cores))

    piece = f32(ff // 128 * rows + 8, 128)
    far, back, near, mine = local(cut_kernel, [piece] * 4, terms, own, own_next, other)
    ring = ("z_hi", "core")
    far = lax.ppermute(far, ring, one_way(layers, cores))
    back = lax.ppermute(back, ring, one_way(layers, cores, -1))
    near = local(add_kernel, [piece], near, far)
    near = lax.ppermute(near, ring, one_way(layers, cores))

    folded = fold(over_x)
    over_z = lax.all_to_all(folded.reshape(nz, own_rows, dw), "z_lo", 0, 0, tiled=True)
    state = f32(rows, ff)
    old = local(state_kernel, [state] * 3, master, moment, second)
    return local(
        functools.partial(last_step_kernel, replicas, group_rows),
        [bf16(own_rows, dw), bf16(group_rows, ff), state, state, state],
        mine, near, back, over_z, up_part, *old,
    )


def solution(mesh):
    split = Mesh(mesh.devices.reshape(4, 8, 2, 4, 4), REPLICA + SHARD)
    return jax.shard_map(
        on_device,
        mesh=split,
        in_specs=(
            P(REPLICA, None),
            P(REPLICA, SHARD),
            P(REPLICA, SHARD),
            P(REPLICA, SHARD),
            P(REPLICA, None),
            P(REPLICA, None),
            P(None, SHARD),
            P(REPLICA, SHARD),
            P(REPLICA, SHARD),
            P(REPLICA, SHARD),
        ),
        out_specs=(
            P(REPLICA + SHARD, None),
            P(REPLICA, SHARD),
            P(REPLICA, SHARD),
            P(REPLICA, SHARD),
            P(REPLICA, SHARD),
        ),
        check_vma=False,
    )
```

```python
import functools
import math

import jax
import jax.numpy as jnp
from jax import lax
from jax.experimental import pallas as pl
from jax.experimental.pallas import tpu as pltpu
from jax.sharding import Mesh
from jax.sharding import PartitionSpec as P

REPLICA = ("z_hi", "y", "core")
SHARD = ("x", "z_lo")


def swap(cores):
    return [(i, (i + 1) % cores) for i in range(cores)]


def one_way(size, cores, turn=1):
    ways = [turn if c % 2 == 0 else -turn for c in range(cores)]
    return [(i * cores + c, (i + ways[c]) % size * cores + c) for i in range(size) for c in range(cores)]


def silu_parts(gate_pre, hidden_grad, weights):
    gate = gate_pre.astype(jnp.float32)
    sig = 1.0 / (1.0 + jnp.exp(-gate))
    return gate, sig, hidden_grad.astype(jnp.float32) * weights


def front_kernel(
    inputs_hbm, gate_hbm, up_hbm, hidden_hbm, seg_hbm, doc_hbm, w_hbm,
    send_far, send_rest, keep_far, keep_rest, part_hbm, up_part_hbm,
    inputs_ref, gate_ref, up_ref, hidden_ref, seg_ref, doc_ref, w_ref,
    full_ref, tail_ref, part_ref, up_part_ref, arrived, left,
):
    pairs = (
        (seg_hbm, seg_ref), (doc_hbm, doc_ref), (gate_hbm, gate_ref), (hidden_hbm, hidden_ref),
        (up_hbm, up_ref), (inputs_hbm, inputs_ref), (w_hbm, w_ref),
    )
    copies = [pltpu.make_async_copy(a, b, arrived.at[i]) for i, (a, b) in enumerate(pairs)]
    for copy in copies:
        copy.start()
    y, core = lax.axis_index("y"), lax.axis_index("core")
    layers, blocks, cores, rows, ff = full_ref.shape
    half = blocks // 2
    out = []

    def put(src, dst):
        copy = pltpu.make_async_copy(src, dst, left.at[len(out)])
        copy.start()
        out.append(copy)

    for copy in copies[:2]:
        copy.wait()
    segs = doc_ref.shape[1]
    tokens = seg_ref.shape[1]
    doc = doc_ref[...].astype(jnp.float32)
    row = lax.broadcasted_iota(jnp.int32, (segs, segs), 0)
    col = lax.broadcasted_iota(jnp.int32, (segs, segs), 1)
    doc_col = jnp.sum(jnp.where(row == col, doc, 0.0), axis=1, keepdims=True)
    label = lax.broadcasted_iota(jnp.int32, (segs, tokens), 0)
    onehot = jnp.where(label == seg_ref[...], 1.0, 0.0)
    tail_ref[...] = jnp.full(tail_ref.shape, jnp.sum(onehot * doc_col), jnp.float32)
    wide = lax.dot_general(
        onehot.astype(jnp.bfloat16),
        jnp.broadcast_to(doc_col, (segs, 128)).astype(jnp.bfloat16),
        (((0,), (0,)), ((), ())),
        preferred_element_type=jnp.float32,
    )
    weights = wide[:, :1]
    for copy in copies[2:5]:
        copy.wait()
    gate, sig, weighted = silu_parts(gate_ref[...], hidden_ref[...], weights)
    up = up_ref[...].astype(jnp.float32)
    raw = (weighted * up * sig * (1.0 + gate * (1.0 - sig))).astype(jnp.bfloat16)
    up_part_ref[...] = weighted * gate * sig
    put(up_part_ref, up_part_hbm)
    per = blocks * cores * rows
    sides = []
    for far, rest, side in ((send_far, send_rest, 1 - core), (keep_far, keep_rest, core)):
        way = 1 - 2 * side
        todo = [(far, None, y + half, side)]
        for k in range(half - 1, 0, -1):
            place = 2 * (half - 1 - k)
            todo.append((rest, place, y + way * k, side))
            todo.append((rest, place + 1, y + way * k, 1 - side))
        todo.append((rest, blocks - 2, y, side))
        sides += todo
    copies[5].wait()
    for z in range(layers):
        part = lax.dot_general(
            inputs_ref[:, z * per : (z + 1) * per], raw, (((0,), (0,)), ((), ())),
            preferred_element_type=jnp.float32,
        )
        full_ref[z] = part.reshape(blocks, cores, rows, ff)
        lines = pl.ds(z * rows, rows)
        for ref, place, target, side in sides:
            target = lax.rem(target + blocks, blocks)
            if place is None:
                ref[lines] = full_ref[z, target, side]
            else:
                put(full_ref.at[z, target, side], ref.at[place, lines])
        if z == 0:
            lines = pl.ds(layers * rows, 8)
            for ref, place, _, _ in sides:
                if place is None:
                    ref[lines] = tail_ref[...]
                else:
                    put(tail_ref, ref.at[place, lines])
    copies[6].wait()
    step = w_ref.shape[0] // 4
    for i in range(4):
        cols = pl.ds(i * step, step)
        part_ref[:, cols] = lax.dot_general(
            raw, w_ref[cols], (((1,), (1,)), ((), ())), preferred_element_type=jnp.float32
        )
        put(part_ref.at[:, cols], part_hbm.at[:, cols])
    for copy in out:
        copy.wait()


def add_kernel(own_ref, other_ref, out_ref):
    out_ref[...] = own_ref[...] + other_ref[...]


def rest_kernel(own_ref, other_ref, terms_ref, *first_refs):
    for place, block in enumerate((0, 3, 2)):
        terms_ref[place] = own_ref[block] + other_ref[block]
    for ref, block in zip(first_refs, (1, 5, 4, 6)):
        ref[...] = own_ref[block] + other_ref[block]


def hop_kernel(block, terms_ref, came_ref, out_ref):
    out_ref[...] = terms_ref[block] + came_ref[...]


def cut_kernel(here_ref, came_ref, next_ref, swapped_ref, far_ref, back_ref, near_ref, mine_ref):
    layers = lax.axis_size("z_hi")
    rows = (here_ref.shape[0] - 8) // layers
    z, core = lax.axis_index("z_hi"), lax.axis_index("core")
    way = 1 - 2 * core
    wide = here_ref.shape[1] // 128
    tail = pl.ds(layers * rows, 8)

    def total(part, cols):
        own = came_ref[part, cols] + next_ref[part, cols]
        return here_ref[part, cols] + own + swapped_ref[part, cols]

    count = total(tail, pl.ds(0, 128))
    for out, target in ((far_ref, z + layers // 2), (back_ref, z - way), (near_ref, z + way), (mine_ref, z)):
        start = pl.multiple_of(lax.rem(target + layers, layers) * rows, rows)
        part = pl.ds(start, rows)
        for c in range(wide):
            out[c * rows : (c + 1) * rows] = total(part, pl.ds(c * 128, 128))
        out[wide * rows :] = count


def fold_kernel(pieces_hbm, out_hbm, pieces_ref, out_ref, arrived, left):
    n, rows = pieces_ref.shape[0], pieces_ref.shape[1]
    cuts = left.shape[0]
    step = rows // cuts
    copies, out = [], []
    for i in range(cuts):
        lines = pl.ds(i * step, step)
        copies.append(
            pltpu.make_async_copy(pieces_hbm.at[:, lines], pieces_ref.at[:, lines], arrived.at[i])
        )
        copies[-1].start()
    for i in range(cuts):
        lines = pl.ds(i * step, step)
        copies[i].wait()
        total = pieces_ref[0, lines]
        for k in range(1, n):
            total = total + pieces_ref[k, lines]
        out_ref[lines] = total
        out.append(pltpu.make_async_copy(out_ref.at[lines], out_hbm.at[lines], left.at[i]))
        out[-1].start()
    for copy in out:
        copy.wait()


def state_kernel(master_ref, moment_ref, second_ref, master_out, moment_out, second_out):
    master_out[...] = master_ref[...]
    moment_out[...] = 0.9 * moment_ref[...]
    second_out[...] = 0.95 * second_ref[...]


def last_step_kernel(
    replicas, group_rows, mine_ref, came_ref, back_ref, input_ref, up_ref, master_ref, moment_ref, second_ref,
    input_grad_ref, up_grad_ref, master_out, moment_out, second_out,
):
    rows, ff = master_ref.shape
    wide = ff // 128
    tail = pl.ds(wide * rows, 8)
    count = mine_ref[tail] + came_ref[tail] + back_ref[tail]
    total = count[:1, :1]
    scale = jnp.float32(group_rows * replicas) / total
    group_scale = jnp.float32(group_rows) / total
    input_sum = input_ref[0]
    for k in range(1, input_ref.shape[0]):
        input_sum = input_sum + input_ref[k]
    input_grad_ref[...] = (input_sum * scale).astype(jnp.bfloat16)
    up_grad_ref[...] = (up_ref[...] * scale).astype(jnp.bfloat16)
    for c in range(wide):
        part, cols = pl.ds(c * rows, rows), pl.ds(c * 128, 128)
        grad = (mine_ref[part] + came_ref[part] + back_ref[part]) * group_scale
        moment = moment_ref[:, cols] + 0.1 * grad
        second = second_ref[:, cols] + 0.05 * grad * grad
        moment_out[:, cols] = moment
        second_out[:, cols] = second
        first_fix = moment / (1.0 - 0.9**8)
        second_fix = second / (1.0 - 0.95**8)
        master = master_ref[:, cols]
        master_out[:, cols] = master - 0.003 * (
            first_fix / (jnp.sqrt(second_fix) + 1e-08) + 0.1 * master
        )


def local(kernel, outs, *args, flops=0):
    vmem = pl.BlockSpec(memory_space=pltpu.VMEM)
    moved = sum(math.prod(a.shape) * a.dtype.itemsize for a in (*args, *outs))
    single = len(outs) == 1
    return pl.pallas_call(
        kernel,
        out_shape=outs[0] if single else tuple(outs),
        in_specs=[vmem] * len(args),
        out_specs=vmem if single else (vmem,) * len(outs),
        compiler_params=pltpu.CompilerParams(vmem_limit_bytes=16 * 2**20),
        cost_estimate=pl.CostEstimate(flops=max(flops, moved), bytes_accessed=moved, transcendentals=0),
    )(*args)


def front(inputs, gate_pre, up_pre, hidden_grad, segment_ids, doc_weight, w_gate, sizes):
    layers, blocks, cores = sizes
    tokens, dw = inputs.shape
    ff = gate_pre.shape[1]
    rows = dw // (layers * blocks * cores)
    far, rest = f32(layers * rows + 8, ff), f32(blocks - 1, layers * rows + 8, ff)
    hbm, vmem = pl.BlockSpec(memory_space=pl.ANY), pl.BlockSpec(memory_space=pltpu.VMEM)
    args = (inputs, gate_pre, up_pre, hidden_grad, segment_ids, doc_weight, w_gate)
    return pl.pallas_call(
        front_kernel,
        out_shape=(far, rest, far, rest, f32(tokens, dw), f32(tokens, ff)),
        in_specs=[hbm] * 7,
        out_specs=(vmem, hbm, vmem, hbm, hbm, hbm),
        scratch_shapes=[pltpu.VMEM(a.shape, a.dtype) for a in args]
        + [
            pltpu.VMEM((layers, blocks, cores, rows, ff), jnp.float32),
            pltpu.VMEM((8, ff), jnp.float32),
            pltpu.VMEM((tokens, dw), jnp.float32),
            pltpu.VMEM((tokens, ff), jnp.float32),
            pltpu.SemaphoreType.DMA((7,)),
            pltpu.SemaphoreType.DMA((2 * (layers + 1) * blocks + 5,)),
        ],
        compiler_params=pltpu.CompilerParams(vmem_limit_bytes=56 * 2**20),
        cost_estimate=pl.CostEstimate(
            flops=4 * tokens * dw * ff, bytes_accessed=14 * 2**20, transcendentals=tokens * ff
        ),
        name="front",
    )(*args)


def fold(pieces):
    hbm = pl.BlockSpec(memory_space=pl.ANY)
    out = f32(*pieces.shape[1:])
    cuts = 4
    return pl.pallas_call(
        fold_kernel,
        out_shape=out,
        in_specs=[hbm],
        out_specs=hbm,
        scratch_shapes=[pltpu.VMEM(a.shape, a.dtype) for a in (pieces, out)]
        + [pltpu.SemaphoreType.DMA((cuts,)), pltpu.SemaphoreType.DMA((cuts,))],
        compiler_params=pltpu.CompilerParams(vmem_limit_bytes=56 * 2**20),
        cost_estimate=pl.CostEstimate(flops=2**22, bytes_accessed=5 * 2**19, transcendentals=0),
        name="fold_x",
    )(pieces)


def f32(*shape):
    return jax.ShapeDtypeStruct(shape, jnp.float32)


def bf16(*shape):
    return jax.ShapeDtypeStruct(shape, jnp.bfloat16)


def on_device(
    inputs, gate_pre, up_pre, hidden_grad, segment_ids, doc_weight, w_gate, master, moment, second
):
    group_rows, dw = inputs.shape
    rows, ff = master.shape
    replicas = lax.axis_size(REPLICA)
    layers, blocks, cores = (lax.axis_size(a) for a in REPLICA)
    nx, nz = (lax.axis_size(a) for a in SHARD)
    own_rows = group_rows // (nx * nz)
    send_far, send_rest, keep_far, keep_rest, part, up_part = front(
        inputs, gate_pre, up_pre, hidden_grad, segment_ids, doc_weight, w_gate, (layers, blocks, cores)
    )
    over_x = lax.all_to_all(part.reshape(nx, nz * own_rows, dw), "x", 0, 0, tiled=True)
    got_far = lax.ppermute(send_far, "core", swap(cores))
    got_rest = lax.ppermute(send_rest, "core", swap(cores))

    block = f32(layers * rows + 8, ff)
    ring, one, two = ("y", "core"), one_way(blocks, cores), one_way(blocks, cores, 2)
    own = local(add_kernel, [block], keep_far, got_far)
    own = lax.ppermute(own, ring, one)
    terms, other, other_next, own_next, here = local(
        rest_kernel, [f32(3, layers * rows + 8, ff)] + [block] * 4, keep_rest, got_rest
    )
    other = lax.ppermute(other, ring, one)
    other_next = lax.ppermute(other_next, ring, one)
    own = local(functools.partial(hop_kernel, 0), [block], terms, own)
    own = lax.ppermute(own, ring, one)
    own_next = lax.ppermute(own_next, ring, one)
    other = local(functools.partial(hop_kernel, 1), [block], terms, other)
    other = lax.ppermute(other, ring, two)
    own = local(functools.partial(hop_kernel, 2), [block], terms, own)
    own = lax.ppermute(own, ring, two)
    other = local(add_kernel, [block], other, other_next)
    other = lax.ppermute(other, "core", swap(cores))

    piece = f32(ff // 128 * rows + 8, 128)
    far, back, near, mine = local(cut_kernel, [piece] * 4, here, own, own_next, other)
    ring = ("z_hi", "core")
    far = lax.ppermute(far, ring, one_way(layers, cores))
    back = lax.ppermute(back, "core", swap(cores))
    back = lax.ppermute(back, ring, one_way(layers, cores))
    near = local(add_kernel, [piece], near, far)
    near = lax.ppermute(near, ring, one_way(layers, cores))
    back = lax.ppermute(back, "core", swap(cores))

    folded = fold(over_x)
    over_z = lax.all_to_all(folded.reshape(nz, own_rows, dw), "z_lo", 0, 0, tiled=True)
    state = f32(rows, ff)
    old = local(state_kernel, [state] * 3, master, moment, second)
    return local(
        functools.partial(last_step_kernel, replicas, group_rows),
        [bf16(own_rows, dw), bf16(group_rows, ff), state, state, state],
        mine, near, back, over_z, up_part, *old,
    )


def solution(mesh):
    split = Mesh(mesh.devices.reshape(4, 8, 2, 4, 4), REPLICA + SHARD)
    return jax.shard_map(
        on_device,
        mesh=split,
        in_specs=(
            P(REPLICA, None),
            P(REPLICA, SHARD),
            P(REPLICA, SHARD),
            P(REPLICA, SHARD),
            P(REPLICA, None),
            P(REPLICA, None),
            P(None, SHARD),
            P(REPLICA, SHARD),
            P(REPLICA, SHARD),
            P(REPLICA, SHARD),
        ),
        out_specs=(
            P(REPLICA + SHARD, None),
            P(REPLICA, SHARD),
            P(REPLICA, SHARD),
            P(REPLICA, SHARD),
            P(REPLICA, SHARD),
        ),
        check_vma=False,
    )
```

```python
import functools
import math

import jax
import jax.numpy as jnp
from jax import lax
from jax.experimental import pallas as pl
from jax.experimental.pallas import tpu as pltpu
from jax.sharding import Mesh
from jax.sharding import PartitionSpec as P

REPLICA = ("z_hi", "y", "core")
SHARD = ("x", "z_lo")


def swap(cores):
    return [(i, (i + 1) % cores) for i in range(cores)]


def one_way(size, cores, turn=1):
    ways = [turn if c % 2 == 0 else -turn for c in range(cores)]
    return [(i * cores + c, (i + ways[c]) % size * cores + c) for i in range(size) for c in range(cores)]


def silu_parts(gate_pre, hidden_grad, weights):
    gate = gate_pre.astype(jnp.float32)
    sig = 1.0 / (1.0 + jnp.exp(-gate))
    return gate, sig, hidden_grad.astype(jnp.float32) * weights


def front_kernel(
    inputs_hbm, gate_hbm, up_hbm, hidden_hbm, seg_hbm, doc_hbm, w_hbm,
    send_far, send_rest, keep_far, keep_rest, part_hbm, up_part_hbm,
    inputs_ref, gate_ref, up_ref, hidden_ref, seg_ref, doc_ref, w_ref,
    full_ref, tail_ref, part_ref, up_part_ref, arrived, left,
):
    pairs = (
        (seg_hbm, seg_ref), (doc_hbm, doc_ref), (gate_hbm, gate_ref), (hidden_hbm, hidden_ref),
        (up_hbm, up_ref), (inputs_hbm, inputs_ref), (w_hbm, w_ref),
    )
    copies = [pltpu.make_async_copy(a, b, arrived.at[i]) for i, (a, b) in enumerate(pairs)]
    for copy in copies:
        copy.start()
    y, core = lax.axis_index("y"), lax.axis_index("core")
    layers, blocks, cores, rows, ff = full_ref.shape
    half = blocks // 2
    out = []

    def put(src, dst):
        copy = pltpu.make_async_copy(src, dst, left.at[len(out)])
        copy.start()
        out.append(copy)

    for copy in copies[:2]:
        copy.wait()
    segs = doc_ref.shape[1]
    tokens = seg_ref.shape[1]
    doc = doc_ref[...].astype(jnp.float32)
    row = lax.broadcasted_iota(jnp.int32, (segs, segs), 0)
    col = lax.broadcasted_iota(jnp.int32, (segs, segs), 1)
    doc_col = jnp.sum(jnp.where(row == col, doc, 0.0), axis=1, keepdims=True)
    label = lax.broadcasted_iota(jnp.int32, (segs, tokens), 0)
    onehot = jnp.where(label == seg_ref[...], 1.0, 0.0)
    tail_ref[...] = jnp.full(tail_ref.shape, jnp.sum(onehot * doc_col), jnp.float32)
    wide = lax.dot_general(
        onehot.astype(jnp.bfloat16),
        jnp.broadcast_to(doc_col, (segs, 128)).astype(jnp.bfloat16),
        (((0,), (0,)), ((), ())),
        preferred_element_type=jnp.float32,
    )
    weights = wide[:, :1]
    for copy in copies[2:5]:
        copy.wait()
    gate, sig, weighted = silu_parts(gate_ref[...], hidden_ref[...], weights)
    up = up_ref[...].astype(jnp.float32)
    raw = (weighted * up * sig * (1.0 + gate * (1.0 - sig))).astype(jnp.bfloat16)
    up_part_ref[...] = weighted * gate * sig
    put(up_part_ref, up_part_hbm)
    per = blocks * cores * rows
    sides = []
    for far, rest, side in ((send_far, send_rest, 1 - core), (keep_far, keep_rest, core)):
        way = 1 - 2 * side
        todo = [(far, None, y + half, side)]
        for k in range(half - 1, 0, -1):
            place = 2 * (half - 1 - k)
            todo.append((rest, place, y + way * k, side))
            todo.append((rest, place + 1, y + way * k, 1 - side))
        todo.append((rest, blocks - 2, y, side))
        sides += todo
    copies[5].wait()
    for z in range(layers):
        part = lax.dot_general(
            inputs_ref[:, z * per : (z + 1) * per], raw, (((0,), (0,)), ((), ())),
            preferred_element_type=jnp.float32,
        )
        full_ref[z] = part.reshape(blocks, cores, rows, ff)
        lines = pl.ds(z * rows, rows)
        for ref, place, target, side in sides:
            src = full_ref.at[z, lax.rem(target + blocks, blocks), side]
            put(src, ref.at[lines] if place is None else ref.at[place, lines])
        if z == 0:
            lines = pl.ds(layers * rows, 8)
            for ref, place, _, _ in sides:
                put(tail_ref, ref.at[lines] if place is None else ref.at[place, lines])
    copies[6].wait()
    step = w_ref.shape[0] // 4
    for i in range(4):
        cols = pl.ds(i * step, step)
        part_ref[:, cols] = lax.dot_general(
            raw, w_ref[cols], (((1,), (1,)), ((), ())), preferred_element_type=jnp.float32
        )
        put(part_ref.at[:, cols], part_hbm.at[:, cols])
    for copy in out:
        copy.wait()


def add_kernel(own_ref, other_ref, out_ref):
    out_ref[...] = own_ref[...] + other_ref[...]


def rest_kernel(own_ref, other_ref, terms_ref, *first_refs):
    for place, block in enumerate((0, 3, 2)):
        terms_ref[place] = own_ref[block] + other_ref[block]
    for ref, block in zip(first_refs, (1, 5, 4, 6)):
        ref[...] = own_ref[block] + other_ref[block]


def hop_kernel(block, terms_ref, came_ref, out_ref):
    out_ref[...] = terms_ref[block] + came_ref[...]


def cut_kernel(here_ref, came_ref, next_ref, swapped_ref, far_ref, back_ref, near_ref, mine_ref):
    layers = lax.axis_size("z_hi")
    rows = (here_ref.shape[0] - 8) // layers
    z, core = lax.axis_index("z_hi"), lax.axis_index("core")
    way = 1 - 2 * core
    wide = here_ref.shape[1] // 128
    tail = pl.ds(layers * rows, 8)

    def total(part, cols):
        own = came_ref[part, cols] + next_ref[part, cols]
        return here_ref[part, cols] + own + swapped_ref[part, cols]

    count = total(tail, pl.ds(0, 128))
    for out, target in ((far_ref, z + layers // 2), (back_ref, z - way), (near_ref, z + way), (mine_ref, z)):
        start = pl.multiple_of(lax.rem(target + layers, layers) * rows, rows)
        part = pl.ds(start, rows)
        for c in range(wide):
            out[c * rows : (c + 1) * rows] = total(part, pl.ds(c * 128, 128))
        out[wide * rows :] = count


def fold_kernel(pieces_hbm, out_hbm, pieces_ref, out_ref, arrived, left):
    n, rows = pieces_ref.shape[0], pieces_ref.shape[1]
    cuts = left.shape[0]
    step = rows // cuts
    copies, out = [], []
    for i in range(cuts):
        lines = pl.ds(i * step, step)
        copies.append(
            pltpu.make_async_copy(pieces_hbm.at[:, lines], pieces_ref.at[:, lines], arrived.at[i])
        )
        copies[-1].start()
    for i in range(cuts):
        lines = pl.ds(i * step, step)
        copies[i].wait()
        total = pieces_ref[0, lines]
        for k in range(1, n):
            total = total + pieces_ref[k, lines]
        out_ref[lines] = total
        out.append(pltpu.make_async_copy(out_ref.at[lines], out_hbm.at[lines], left.at[i]))
        out[-1].start()
    for copy in out:
        copy.wait()


def state_kernel(master_ref, moment_ref, second_ref, master_out, moment_out, second_out):
    master_out[...] = master_ref[...]
    moment_out[...] = 0.9 * moment_ref[...]
    second_out[...] = 0.95 * second_ref[...]


def last_step_kernel(
    replicas, group_rows, mine_ref, came_ref, back_ref, input_ref, up_ref, master_ref, moment_ref, second_ref,
    input_grad_ref, up_grad_ref, master_out, moment_out, second_out,
):
    rows, ff = master_ref.shape
    wide = ff // 128
    tail = pl.ds(wide * rows, 8)
    count = mine_ref[tail] + came_ref[tail] + back_ref[tail]
    total = count[:1, :1]
    scale = jnp.float32(group_rows * replicas) / total
    group_scale = jnp.float32(group_rows) / total
    input_sum = input_ref[0]
    for k in range(1, input_ref.shape[0]):
        input_sum = input_sum + input_ref[k]
    input_grad_ref[...] = (input_sum * scale).astype(jnp.bfloat16)
    up_grad_ref[...] = (up_ref[...] * scale).astype(jnp.bfloat16)
    for c in range(wide):
        part, cols = pl.ds(c * rows, rows), pl.ds(c * 128, 128)
        grad = (mine_ref[part] + came_ref[part] + back_ref[part]) * group_scale
        moment = moment_ref[:, cols] + 0.1 * grad
        second = second_ref[:, cols] + 0.05 * grad * grad
        moment_out[:, cols] = moment
        second_out[:, cols] = second
        first_fix = moment / (1.0 - 0.9**8)
        second_fix = second / (1.0 - 0.95**8)
        master = master_ref[:, cols]
        master_out[:, cols] = master - 0.003 * (
            first_fix / (jnp.sqrt(second_fix) + 1e-08) + 0.1 * master
        )


def local(kernel, outs, *args, flops=0):
    vmem = pl.BlockSpec(memory_space=pltpu.VMEM)
    moved = sum(math.prod(a.shape) * a.dtype.itemsize for a in (*args, *outs))
    single = len(outs) == 1
    return pl.pallas_call(
        kernel,
        out_shape=outs[0] if single else tuple(outs),
        in_specs=[vmem] * len(args),
        out_specs=vmem if single else (vmem,) * len(outs),
        compiler_params=pltpu.CompilerParams(vmem_limit_bytes=16 * 2**20),
        cost_estimate=pl.CostEstimate(flops=max(flops, moved), bytes_accessed=moved, transcendentals=0),
    )(*args)


def front(inputs, gate_pre, up_pre, hidden_grad, segment_ids, doc_weight, w_gate, sizes):
    layers, blocks, cores = sizes
    tokens, dw = inputs.shape
    ff = gate_pre.shape[1]
    rows = dw // (layers * blocks * cores)
    far, rest = f32(layers * rows + 8, ff), f32(blocks - 1, layers * rows + 8, ff)
    hbm = pl.BlockSpec(memory_space=pl.ANY)
    args = (inputs, gate_pre, up_pre, hidden_grad, segment_ids, doc_weight, w_gate)
    return pl.pallas_call(
        front_kernel,
        out_shape=(far, rest, far, rest, f32(tokens, dw), f32(tokens, ff)),
        in_specs=[hbm] * 7,
        out_specs=(hbm,) * 6,
        scratch_shapes=[pltpu.VMEM(a.shape, a.dtype) for a in args]
        + [
            pltpu.VMEM((layers, blocks, cores, rows, ff), jnp.float32),
            pltpu.VMEM((8, ff), jnp.float32),
            pltpu.VMEM((tokens, dw), jnp.float32),
            pltpu.VMEM((tokens, ff), jnp.float32),
            pltpu.SemaphoreType.DMA((7,)),
            pltpu.SemaphoreType.DMA((2 * (layers + 1) * blocks + 5,)),
        ],
        compiler_params=pltpu.CompilerParams(vmem_limit_bytes=56 * 2**20),
        cost_estimate=pl.CostEstimate(
            flops=4 * tokens * dw * ff, bytes_accessed=14 * 2**20, transcendentals=tokens * ff
        ),
        name="front",
    )(*args)


def fold(pieces):
    hbm = pl.BlockSpec(memory_space=pl.ANY)
    out = f32(*pieces.shape[1:])
    cuts = 4
    return pl.pallas_call(
        fold_kernel,
        out_shape=out,
        in_specs=[hbm],
        out_specs=hbm,
        scratch_shapes=[pltpu.VMEM(a.shape, a.dtype) for a in (pieces, out)]
        + [pltpu.SemaphoreType.DMA((cuts,)), pltpu.SemaphoreType.DMA((cuts,))],
        compiler_params=pltpu.CompilerParams(vmem_limit_bytes=56 * 2**20),
        cost_estimate=pl.CostEstimate(flops=2**22, bytes_accessed=5 * 2**19, transcendentals=0),
        name="fold_x",
    )(pieces)


def f32(*shape):
    return jax.ShapeDtypeStruct(shape, jnp.float32)


def bf16(*shape):
    return jax.ShapeDtypeStruct(shape, jnp.bfloat16)


def on_device(
    inputs, gate_pre, up_pre, hidden_grad, segment_ids, doc_weight, w_gate, master, moment, second
):
    group_rows, dw = inputs.shape
    rows, ff = master.shape
    replicas = lax.axis_size(REPLICA)
    layers, blocks, cores = (lax.axis_size(a) for a in REPLICA)
    nx, nz = (lax.axis_size(a) for a in SHARD)
    own_rows = group_rows // (nx * nz)
    send_far, send_rest, keep_far, keep_rest, part, up_part = front(
        inputs, gate_pre, up_pre, hidden_grad, segment_ids, doc_weight, w_gate, (layers, blocks, cores)
    )
    over_x = lax.all_to_all(part.reshape(nx, nz * own_rows, dw), "x", 0, 0, tiled=True)
    got_far = lax.ppermute(send_far, "core", swap(cores))
    got_rest = lax.ppermute(send_rest, "core", swap(cores))

    block = f32(layers * rows + 8, ff)
    ring, one, two = ("y", "core"), one_way(blocks, cores), one_way(blocks, cores, 2)
    own = local(add_kernel, [block], keep_far, got_far)
    own = lax.ppermute(own, ring, one)
    terms, other, other_next, own_next, here = local(
        rest_kernel, [f32(3, layers * rows + 8, ff)] + [block] * 4, keep_rest, got_rest
    )
    other = lax.ppermute(other, ring, one)
    other_next = lax.ppermute(other_next, ring, one)
    own = local(functools.partial(hop_kernel, 0), [block], terms, own)
    own = lax.ppermute(own, ring, one)
    own_next = lax.ppermute(own_next, ring, one)
    other = local(functools.partial(hop_kernel, 1), [block], terms, other)
    other = lax.ppermute(other, ring, two)
    own = local(functools.partial(hop_kernel, 2), [block], terms, own)
    own = lax.ppermute(own, ring, two)
    other = local(add_kernel, [block], other, other_next)
    other = lax.ppermute(other, "core", swap(cores))

    piece = f32(ff // 128 * rows + 8, 128)
    far, back, near, mine = local(cut_kernel, [piece] * 4, here, own, own_next, other)
    ring = ("z_hi", "core")
    far = lax.ppermute(far, ring, one_way(layers, cores))
    back = lax.ppermute(back, "core", swap(cores))
    back = lax.ppermute(back, ring, one_way(layers, cores))
    near = local(add_kernel, [piece], near, far)
    near = lax.ppermute(near, ring, one_way(layers, cores))
    back = lax.ppermute(back, "core", swap(cores))

    folded = fold(over_x)
    over_z = lax.all_to_all(folded.reshape(nz, own_rows, dw), "z_lo", 0, 0, tiled=True)
    state = f32(rows, ff)
    old = local(state_kernel, [state] * 3, master, moment, second)
    return local(
        functools.partial(last_step_kernel, replicas, group_rows),
        [bf16(own_rows, dw), bf16(group_rows, ff), state, state, state],
        mine, near, back, over_z, up_part, *old,
    )


def solution(mesh):
    split = Mesh(mesh.devices.reshape(4, 8, 2, 4, 4), REPLICA + SHARD)
    return jax.shard_map(
        on_device,
        mesh=split,
        in_specs=(
            P(REPLICA, None),
            P(REPLICA, SHARD),
            P(REPLICA, SHARD),
            P(REPLICA, SHARD),
            P(REPLICA, None),
            P(REPLICA, None),
            P(None, SHARD),
            P(REPLICA, SHARD),
            P(REPLICA, SHARD),
            P(REPLICA, SHARD),
        ),
        out_specs=(
            P(REPLICA + SHARD, None),
            P(REPLICA, SHARD),
            P(REPLICA, SHARD),
            P(REPLICA, SHARD),
            P(REPLICA, SHARD),
        ),
        check_vma=False,
    )
```
